32 devices in a mesh: section: 4 (over y, x), tensor: 2 (over core), dp: 4 (over z).
Axes of the slice: x: 2, y: 2, z: 4, core: 2. Of those that a mesh axis runs over, the one named last changes fastest.
Arguments:
- hidden_in: bfloat16 [128, 4096], P('dp', 'tensor'), may hold values from -6 to 6
- norm_gain: float32 [4, 4096], P('section'), may hold values from 0.25 to 1.75
- gate_weight: bfloat16 [4, 4096, 8192], P('section', 'dp', 'tensor'), may hold values from -0.09375 to 0.09375
- up_weight: bfloat16 [4, 4096, 8192], P('section', 'dp', 'tensor'), may hold values from -0.09375 to 0.09375
- down_weight: bfloat16 [4, 4096, 8192], P('section', 'dp', 'tensor'), may hold values from -0.0625 to 0.0625
- lengths: int32 [16], P('dp'), may hold values from 3 to 8
Outputs:
- rdm: float32 [4, 16, 16], P('section', 'dp')
The draws below stay inside these ranges and needn't reach their ends.
Inputs may be any that keep to these rules, and one draw needn't show every extreme that they name: `lengths`: the number of leading valid token rows of each sentence.
All inputs are finite; a program needn't handle non-finite values.
Results may differ from the reference program's by a relative error of at most 0.0012.
Values may be sent and summed in bfloat16 or wider, within the bound.
No kernel may reach another device: no remote copies, remote signals or barrier semaphores. Data moves between devices by JAX's collectives and lax.ppermute only.
A program may use at most 192 MiB of HBM per device.

```python
import jax
import jax.numpy as jnp
from jax import lax

D = 4096
FF = 8192
LEN = 8
SENT = 16
TOKENS = 128
SECTIONS = 4
N_SECTION = 4


def plant(drawn, own_key, smallest, top_value):
    longest = drawn.shape.index(max(drawn.shape))
    spots = []
    for shift in (0, 1):
        where = [jax.random.randint(jax.random.fold_in(own_key, axis), (), 0, length) for axis, length in enumerate(drawn.shape)]
        where[longest] = (where[longest] + shift) % drawn.shape[longest]
        spots.append(tuple(where))
    return drawn.at[spots[0]].set(smallest).at[spots[1]].set(top_value)


def block_scale(own_key, shape, pieces, least, largest):
    loudness, own = 1.0, jax.random.fold_in(own_key, 6)
    for axis_at, parts in pieces:
        draws = jnp.exp(jax.random.uniform(jax.random.fold_in(own, axis_at), (parts,), jnp.float32, least / len(pieces), largest / len(pieces)))
        loudness = loudness * jnp.repeat(draws, shape[axis_at] // parts).reshape([-1 if axis == axis_at else 1 for axis in range(len(shape))])
    return loudness


def gaussian(stream_key, dims, deviation, most, split=(), kind=jnp.bfloat16):
    values = deviation * jax.random.normal(stream_key, dims, jnp.float32)
    if split:
        values = values * block_scale(stream_key, dims, split, -0.22, 0.18)
    return jnp.clip(values, -most, most).astype(kind)


def setup_inputs(seed: int = 0) -> dict:
    keys = jax.random.split(jax.random.key(seed), 7)
    return {
        "hidden_in": gaussian(keys[0], (TOKENS, D), 1.0, 6.0, ((0, 4), (1, 2))),
        "norm_gain": jnp.clip(1.0 + 0.15 * jax.random.normal(keys[1], (SECTIONS, D), jnp.float32), 0.25, 1.75),
        "gate_weight": gaussian(keys[2], (SECTIONS, D, FF), D ** -0.5, 0.09375, ((0, 4), (1, 4), (2, 2))),
        "up_weight": gaussian(keys[3], (SECTIONS, D, FF), D ** -0.5, 0.09375, ((0, 4), (1, 4), (2, 2))),
        "down_weight": gaussian(keys[4], (SECTIONS, D, FF), FF ** -0.5, 0.0625, ((0, 4), (1, 4), (2, 2))),
        "lengths": plant(jax.random.randint(keys[5], (SENT,), 3, LEN + 1), jax.random.fold_in(keys[5], 1), 3, LEN).astype(jnp.int32),
    }


RMS_EPS = 1e-05
UNIT_FLOOR = 0.1
CONTRACT_LAST = (((1,), (1,)), ((), ()))

def reference(hidden_in, norm_gain, gate_weight, up_weight, down_weight, lengths):
    current = hidden_in
    positions = jnp.arange(LEN, dtype=jnp.int32)
    weights = (positions[None, :] < lengths[:, None]).astype(jnp.float32)
    counts = lengths.astype(jnp.float32)
    results = []
    for layer in range(N_SECTION):
        wide_state = current.astype(jnp.float32)
        inv_rms = lax.rsqrt(lax.optimization_barrier(jnp.mean(wide_state * wide_state, axis=1, keepdims=True)) + RMS_EPS)
        normed = (wide_state * inv_rms * norm_gain[layer][None, :]).astype(jnp.bfloat16)
        gate_sum = jnp.dot(normed, gate_weight[layer], preferred_element_type=jnp.float32)
        up_sum = jnp.dot(normed, up_weight[layer], preferred_element_type=jnp.float32)
        hidden = (jax.nn.silu(gate_sum) * up_sum).astype(jnp.bfloat16)
        summed = lax.dot_general(hidden, down_weight[layer], CONTRACT_LAST, preferred_element_type=jnp.float32)
        current = (wide_state + summed).astype(jnp.bfloat16)
        shaped = current.astype(jnp.float32).reshape(SENT, LEN, D)
        pooled = lax.optimization_barrier(jnp.sum(shaped * weights[:, :, None], axis=1)) / counts[:, None]
        centered = pooled - lax.optimization_barrier(jnp.mean(pooled, axis=1, keepdims=True))
        unit_rows = (centered * lax.rsqrt(lax.optimization_barrier(jnp.mean(centered * centered, axis=1, keepdims=True)) + UNIT_FLOOR)).astype(jnp.bfloat16)
        products = lax.dot_general(unit_rows, unit_rows, CONTRACT_LAST, preferred_element_type=jnp.float32)
        results.append(1.0 - products / D)
    return jnp.stack(results)
```

```python
import jax
import jax.numpy as jnp
from jax import lax
from jax.sharding import PartitionSpec as P

MICRO = 2
CHUNKS = 2
RMS_EPS = 1e-05
UNIT_FLOOR = 0.1
CONTRACT_LAST = (((1,), (1,)), ((), ()))


def shifted(array, axis, by):
    peers = lax.axis_size(axis)
    return lax.ppermute(array, axis, [(i, (i + by) % peers) for i in range(peers)])


def over_tensor(part):
    if lax.axis_size("tensor") == 2:
        return part.astype(jnp.float32) + shifted(part, "tensor", 1).astype(jnp.float32)
    return lax.psum(part.astype(jnp.float32), "tensor")


def per_device(hidden_in, norm_gain, gate_weight, up_weight, down_weight, lengths):
    section = lax.axis_index("section")
    own = lax.axis_index("dp")
    sections, peers = lax.axis_size("section"), lax.axis_size("dp")
    gate_own, up_own, down_own = gate_weight[0], up_weight[0], down_weight[0]
    width, units = gate_own.shape
    features = width * peers
    rows_own = hidden_in.shape[0]
    held = lengths.shape[0]
    slots = rows_own // held
    rows = rows_own // MICRO
    batch = rows * peers
    sentences = held // MICRO
    piece = units // CHUNKS
    gain = lax.dynamic_slice_in_dim(norm_gain[0], own * width, width, 0)

    entering = lax.all_gather(hidden_in, "tensor", axis=1, tiled=True)
    entering = lax.all_to_all(
        entering.reshape(rows_own, peers, width), "dp", split_axis=1, concat_axis=0, tiled=False
    )
    entering = entering.reshape(peers, MICRO, rows, width)
    all_lengths = lax.all_gather(lengths, "dp", axis=0, tiled=True).reshape(peers, MICRO, sentences)

    def block(array, by):
        return lax.dynamic_slice_in_dim(array, ((own + by) % peers) * rows, rows, 0)

    def layer(current):
        wide = current.astype(jnp.float32)
        squares = jnp.sum(wide * wide, axis=1, keepdims=True)
        total = block(squares, 0)
        for by in range(1, peers):
            total = total + shifted(block(squares, by), "dp", by)
        inv_rms = lax.rsqrt(total / features + RMS_EPS)
        scaled = (wide * gain[None, :]).astype(jnp.bfloat16)
        partial_sum = jnp.zeros((batch, width), jnp.float32)
        for c in range(CHUNKS):
            cut = slice(c * piece, (c + 1) * piece)
            gate_part = jnp.dot(scaled, gate_own[:, cut], preferred_element_type=jnp.float32)
            up_part = jnp.dot(scaled, up_own[:, cut], preferred_element_type=jnp.float32)
            both = jnp.concatenate([gate_part, up_part], axis=1).astype(jnp.bfloat16)
            summed = block(both, 0).astype(jnp.float32)
            for by in range(1, peers):
                summed = summed + shifted(block(both, by), "dp", by).astype(jnp.float32)
            summed = summed * inv_rms
            hidden = (jax.nn.silu(summed[:, :piece]) * summed[:, piece:]).astype(jnp.bfloat16)
            everyone = jnp.concatenate(
                [hidden] + [shifted(hidden, "dp", peers - by) for by in range(1, peers)], axis=0
            )
            partial_sum = partial_sum + lax.dot_general(
                everyone, down_own[:, cut], CONTRACT_LAST, preferred_element_type=jnp.float32
            )
        partial_sum = over_tensor(partial_sum.astype(jnp.bfloat16))
        twice = jnp.concatenate([partial_sum, partial_sum], axis=0)
        partial_sum = lax.dynamic_slice_in_dim(twice, ((peers - own) % peers) * rows, batch, 0)
        return (wide + partial_sum).astype(jnp.bfloat16)

    positions = jnp.arange(slots, dtype=jnp.int32)
    pooled_at = []
    incoming = None
    ticks = MICRO + sections - 1
    for tick in range(ticks):
        if tick == 0:
            current = entering[:, 0].reshape(batch, width)
        elif tick < MICRO:
            current = jnp.where(section == 0, entering[:, tick].reshape(batch, width), incoming)
        else:
            current = incoming
        output = layer(current)
        if tick + 1 < ticks:
            incoming = lax.ppermute(output, "section", [(i, i + 1) for i in range(sections - 1)])
        micro = jnp.clip(tick - section, 0, MICRO - 1)
        valid = lax.dynamic_slice_in_dim(all_lengths, micro, 1, 1).reshape(peers * sentences)
        keep = (positions[None, :] < valid[:, None]).astype(jnp.float32)
        shaped = output.astype(jnp.float32).reshape(peers * sentences, slots, width)
        pooled_at.append(
            jnp.sum(shaped * keep[:, :, None], axis=1) / valid.astype(jnp.float32)[:, None]
        )
    pooled = lax.dynamic_slice_in_dim(jnp.stack(pooled_at), section, MICRO, 0)
    everything = peers * held
    pooled = pooled.reshape(MICRO, peers, sentences, width).transpose(1, 0, 2, 3)
    pooled = pooled.reshape(everything, width)
    middle = jnp.mean(pooled, axis=1, keepdims=True)
    centered = pooled - middle
    gram = lax.dot_general(
        centered, centered, CONTRACT_LAST,
        precision=lax.Precision.HIGHEST, preferred_element_type=jnp.float32,
    )
    packed = lax.all_gather(jnp.concatenate([gram, middle], axis=1), "dp", axis=0, tiled=False)
    grams, middles = packed[:, :, :everything], packed[:, :, everything]
    offsets = middles - jnp.mean(middles, axis=0, keepdims=True)
    whole = jnp.sum(grams + width * offsets[:, :, None] * offsets[:, None, :], axis=0)
    diagonal = jnp.sum(jnp.where(jnp.eye(everything, dtype=bool), whole, 0.0), axis=1)
    scale = lax.rsqrt(diagonal / features + UNIT_FLOOR)
    result = 1.0 - whole * scale[:, None] * scale[None, :] / features
    return lax.dynamic_slice_in_dim(result, own * held, held, 0)[None]


def solution(mesh):
    placed = (
        P("dp", "tensor"),
        P("section", None),
        P("section", "dp", "tensor"),
        P("section", "dp", "tensor"),
        P("section", "dp", "tensor"),
        P("dp"),
    )
    return jax.shard_map(
        per_device, mesh=mesh, in_specs=placed, out_specs=P("section", "dp", None), check_vma=False
    )
```
